32 devices in a mesh: depth: 32 (over z, y, x, core).
Axes of the slice: x: 2, y: 2, z: 4, core: 2. Of those that a mesh axis runs over, the one named last changes fastest.
Arguments:
- weights: bfloat16 [32, 1024, 1024], P('depth'), may hold values from -0.1875 to 0.1875
- gains: float32 [32, 1024], P('depth'), may hold values from 0.1 to 1.9
- states: float32 [32, 512, 1024], P('depth'), may hold values from -1200 to 1200
- adjoints: float32 [32, 512, 1024], P('depth'), may hold values from -0.26516503 to 0.26516503
Outputs:
- grad_weight: bfloat16 [32, 1024, 1024], P('depth')
- grad_gain: float32 [32, 1024], P('depth')
The draws below stay inside these ranges and needn't reach their ends.
All inputs are finite; a program needn't handle non-finite values.
Results may differ from the reference program's by a relative error of at most 0.006.
Values sent between devices are 32-bit elements; how exact they have to be, the bound alone decides.
No kernel may reach another device: no remote copies, remote signals or barrier semaphores. Data moves between devices by JAX's collectives and lax.ppermute only.
A program may use at most 64 MiB of HBM per device.

```python
import math
import jax
import jax.numpy as jnp
from jax import lax

D = 1024
TOK = 512
SWEEPS = 4
LAYERS = 32


def draw_states(key, part):
    first_key, second_key, third_key = jax.random.split(jax.random.fold_in(key, 17), 3)
    noise_vals = jnp.clip(jax.random.normal(first_key, (LAYERS, TOK, D), jnp.float32), -6.0, 6.0)
    upper_scale = 10.0
    row_scale = jnp.exp(jax.random.uniform(second_key, (LAYERS, TOK, 1), jnp.float32, 0.0, math.log(upper_scale)))
    col_scale = jnp.exp(jax.random.uniform(third_key, (LAYERS, 1, D), jnp.float32, 0.0, math.log(upper_scale)))
    return jnp.clip(noise_vals * row_scale * col_scale, -1200.0, 1200.0)


def levels(key, extent, pieces, low, top_value):
    def one(dim, blocks):
        draws = jax.random.uniform(jax.random.fold_in(jax.random.fold_in(key, 6), dim), (blocks,), jnp.float32, low / len(pieces), top_value / len(pieces))
        return jnp.repeat(jnp.exp(draws), extent[dim] // blocks).reshape((-1,) + (1,) * (len(extent) - dim - 1))

    level = one(*pieces[0])
    for cut in pieces[1:]:
        level = level * one(*cut)
    return level


def normal_values(rng, extent, deviation, reach, cuts=(), held_as=jnp.bfloat16):
    values = deviation * jax.random.normal(rng, extent, jnp.float32)
    if cuts:
        values = values * levels(rng, extent, cuts, -0.22, 0.18)
    return jnp.clip(values, -reach, reach).astype(held_as)


def setup_inputs(seed: int = 0) -> dict:
    streams_of = jax.random.split(jax.random.key(seed), 5)
    weights = normal_values(streams_of[0], (LAYERS, D, D), D ** -0.5, 0.1875, ((0, 32),))
    gains = jnp.clip(1.0 + 0.18 * jax.random.normal(streams_of[1], (LAYERS, D), jnp.float32), 0.1, 1.9)
    states = draw_states(jax.random.fold_in(streams_of[4], 71), 0)
    adjoints = normal_values(streams_of[3], (LAYERS, TOK, D), (TOK ** -0.5), 0.26516503, ((0, 32),), jnp.float32)
    return {"weights": weights, "gains": gains, "states": states, "adjoints": adjoints}


eps = 1e-06

def layer_terms(state, adjoint, gains, weights):
    inverse = lax.rsqrt(lax.optimization_barrier(jnp.mean(state * state, axis=-1, keepdims=True)) + eps)
    normed = state * inverse
    scaled = (normed * gains[:, None, :]).astype(jnp.bfloat16)
    preact = jnp.einsum('ltd,lde->lte', scaled.astype(jnp.float32), weights.astype(jnp.float32))
    squash = jax.nn.sigmoid(preact)
    output = state + preact * squash
    pre_grad = (adjoint * squash * (1.0 + preact * (1.0 - squash))).astype(jnp.bfloat16)
    feat_grad = jnp.einsum('lte,lde->ltd', pre_grad.astype(jnp.float32), weights.astype(jnp.float32))
    gained = feat_grad * gains[:, None, :]
    carried = adjoint + inverse * (gained - normed * lax.optimization_barrier(jnp.mean(gained * normed, axis=-1, keepdims=True)))
    return (output, carried, scaled, pre_grad, normed, feat_grad)

def reference(weights, gains, states, adjoints):
    state, adjoint = (states, adjoints)
    for sweep_index in range(SWEEPS):
        output, carried, scaled, pre_grad, normed, feat_grad = layer_terms(state, adjoint, gains, weights)
        state = jnp.concatenate([state[:1], output[:-1]], axis=0)
        adjoint = jnp.concatenate([carried[1:], adjoint[-1:]], axis=0)
    output, carried, scaled, pre_grad, normed, feat_grad = layer_terms(state, adjoint, gains, weights)
    grad_weight = jnp.einsum('ltd,lte->lde', scaled.astype(jnp.float32), pre_grad.astype(jnp.float32)).astype(jnp.bfloat16)
    grad_gain = lax.optimization_barrier(jnp.sum(normed * feat_grad, axis=1))
    return (grad_weight, grad_gain)
```

```python
import jax
import jax.numpy as jnp
from jax import lax
from jax.experimental import pallas as pl
from jax.experimental.pallas import tpu as pltpu
from jax.sharding import PartitionSpec as P


SWEEPS = 4
SHIFTS = (-16, 16)
CHUNKS = len(SHIFTS)

eps = 1e-06


def passed_along(block, axis, distance):
    devices = range(lax.axis_size(axis))
    route = [(i - distance, i) for i in devices if i - distance in devices]
    return lax.ppermute(block, axis, route)


def tick_kernel(x_ref, o_ref):
    o_ref[...] = x_ref[...]


def tick(x):
    return pl.pallas_call(
        tick_kernel,
        out_shape=jax.ShapeDtypeStruct(x.shape, x.dtype),
        in_specs=[pl.BlockSpec(memory_space=pltpu.VMEM)],
        out_specs=pl.BlockSpec(memory_space=pltpu.VMEM),
        name="tick",
    )(x)


def forward_terms(state, gain, weight):
    inverse = lax.rsqrt(jnp.mean(state * state, axis=-1, keepdims=True) + eps)
    normed = state * inverse
    scaled = (normed * gain).astype(jnp.bfloat16)
    preact = jnp.dot(scaled, weight, preferred_element_type=jnp.float32)
    return inverse, normed, scaled, preact, jax.nn.sigmoid(preact)


def backward_terms(adjoint, preact, squash, weight):
    pre_grad = (adjoint * squash * (1.0 + preact * (1.0 - squash))).astype(jnp.bfloat16)
    feat_grad = lax.dot_general(
        pre_grad, weight, (((1,), (1,)), ((), ())), preferred_element_type=jnp.float32
    )
    return pre_grad, feat_grad


def on_device(weights, gains, states, adjoints):
    weight = weights[0]
    turn = gains
    count = lax.axis_size("depth")
    index = lax.axis_index("depth")
    is_first = index == 0
    is_last = index == count - 1
    rows = [states.shape[1] // CHUNKS + shift for shift in SHIFTS]
    cuts = [sum(rows[:c]) for c in range(CHUNKS + 1)]
    start_states = [states[0, cuts[c] : cuts[c + 1]] for c in range(CHUNKS)]
    start_adjoints = [adjoints[0, cuts[c] : cuts[c + 1]] for c in range(CHUNKS)]
    state = list(start_states)
    adjoint = list(start_adjoints)
    for _ in range(SWEEPS):
        for c in range(CHUNKS):
            s, a, turn = lax.optimization_barrier((state[c], adjoint[c], turn))
            inverse, normed, scaled, preact, squash = forward_terms(s, turn, weight)
            output = s + preact * squash
            pre_grad, feat_grad = backward_terms(a, preact, squash, weight)
            gained = feat_grad * turn
            carried = a + inverse * (
                gained - normed * jnp.mean(gained * normed, axis=-1, keepdims=True)
            )
            output, carried, turn = lax.optimization_barrier((output, carried, turn))
            arrived = passed_along(output, "depth", 1)
            arrived_adjoint = passed_along(carried, "depth", -1)
            turn = tick(turn)
            state[c] = jnp.where(is_first, start_states[c], arrived)
            adjoint[c] = jnp.where(is_last, start_adjoints[c], arrived_adjoint)
    total = 0.0
    gain_total = 0.0
    for c in range(CHUNKS):
        s, a, turn = lax.optimization_barrier((state[c], adjoint[c], turn))
        inverse, normed, scaled, preact, squash = forward_terms(s, turn, weight)
        pre_grad, feat_grad = backward_terms(a, preact, squash, weight)
        total = total + lax.dot_general(
            scaled, pre_grad, (((0,), (0,)), ((), ())), preferred_element_type=jnp.float32
        )
        gain_total = gain_total + jnp.sum(normed * feat_grad, axis=0)
        total, turn, gain_total = lax.optimization_barrier((total, turn, gain_total))
        if c < CHUNKS - 1:
            turn = tick(turn)
    return (total.astype(jnp.bfloat16)[None], gain_total[None])


def solution(mesh):
    placed = (
        P("depth", None, None),
        P("depth", None),
        P("depth", None, None),
        P("depth", None, None),
    )
    return jax.shard_map(
        on_device,
        mesh=mesh,
        in_specs=placed,
        out_specs=(P("depth", None, None), P("depth", None)),
        check_vma=False,
    )
```

```python
import jax
import jax.numpy as jnp
from jax import lax
from jax.experimental import pallas as pl
from jax.experimental.pallas import tpu as pltpu
from jax.sharding import PartitionSpec as P


SWEEPS = 4
SHARES = (8, 14, 10)
CHUNKS = len(SHARES)

eps = 1e-06


def swapped(block, axis, first):
    count = lax.axis_size(axis)
    route = []
    for i in range(first, count - 1, 2):
        route += [(i, i + 1), (i + 1, i)]
    return lax.ppermute(block, axis, route)


def tick_kernel(x_ref, o_ref):
    o_ref[...] = x_ref[...]


def tick(x):
    return pl.pallas_call(
        tick_kernel,
        out_shape=jax.ShapeDtypeStruct(x.shape, x.dtype),
        in_specs=[pl.BlockSpec(memory_space=pltpu.VMEM)],
        out_specs=pl.BlockSpec(memory_space=pltpu.VMEM),
        name="tick",
        compiler_params=pltpu.CompilerParams(vmem_limit_bytes=256 * 1024),
    )(x)


def forward_terms(state, gain, weight):
    inverse = lax.rsqrt(jnp.mean(state * state, axis=-1, keepdims=True) + eps)
    normed = state * inverse
    scaled = (normed * gain).astype(jnp.bfloat16)
    preact = jnp.dot(scaled, weight, preferred_element_type=jnp.float32)
    return inverse, normed, scaled, preact, jax.nn.sigmoid(preact)


def backward_terms(adjoint, preact, squash, weight):
    pre_grad = (adjoint * squash * (1.0 + preact * (1.0 - squash))).astype(jnp.bfloat16)
    feat_grad = lax.dot_general(
        pre_grad, weight, (((1,), (1,)), ((), ())), preferred_element_type=jnp.float32
    )
    return pre_grad, feat_grad


def on_device(weights, gains, states, adjoints):
    weight = weights[0]
    turn = gains
    count = lax.axis_size("depth")
    index = lax.axis_index("depth")
    is_first = index == 0
    is_last = index == count - 1
    is_even = index % 2 == 0
    unit = states.shape[1] // sum(SHARES)
    rows = [share * unit for share in SHARES]
    cuts = [sum(rows[:c]) for c in range(CHUNKS + 1)]
    start_states = [states[0, cuts[c] : cuts[c + 1]] for c in range(CHUNKS)]
    start_adjoints = [adjoints[0, cuts[c] : cuts[c + 1]] for c in range(CHUNKS)]
    state = list(start_states)
    adjoint = list(start_adjoints)
    for _ in range(SWEEPS):
        for c in range(CHUNKS):
            s, a, turn = lax.optimization_barrier((state[c], adjoint[c], turn))
            inverse, normed, scaled, preact, squash = forward_terms(s, turn, weight)
            output = s + preact * squash
            pre_grad, feat_grad = backward_terms(a, preact, squash, weight)
            gained = feat_grad * turn
            carried = a + inverse * (
                gained - normed * jnp.mean(gained * normed, axis=-1, keepdims=True)
            )
            near = jnp.where(is_even, output, carried)
            far = jnp.where(is_even, carried, output)
            near, far, turn = lax.optimization_barrier((near, far, turn))
            near = swapped(near, "depth", 0)
            far = swapped(far, "depth", 1)
            turn = tick(turn)
            state[c] = jnp.where(
                is_first, start_states[c], jnp.where(is_even, far, near)
            )
            adjoint[c] = jnp.where(
                is_last, start_adjoints[c], jnp.where(is_even, near, far)
            )
    total = 0.0
    gain_total = 0.0
    for c in range(CHUNKS):
        s, a, turn = lax.optimization_barrier((state[c], adjoint[c], turn))
        inverse, normed, scaled, preact, squash = forward_terms(s, turn, weight)
        pre_grad, feat_grad = backward_terms(a, preact, squash, weight)
        total = total + lax.dot_general(
            scaled, pre_grad, (((0,), (0,)), ((), ())), preferred_element_type=jnp.float32
        )
        gain_total = gain_total + jnp.sum(normed * feat_grad, axis=0)
        if c < CHUNKS - 1:
            total, turn, gain_total = lax.optimization_barrier((total, turn, gain_total))
            turn = tick(turn)
    return (total.astype(jnp.bfloat16)[None], gain_total[None])


def solution(mesh):
    placed = (
        P("depth", None, None),
        P("depth", None),
        P("depth", None, None),
        P("depth", None, None),
    )
    return jax.shard_map(
        on_device,
        mesh=mesh,
        in_specs=placed,
        out_specs=(P("depth", None, None), P("depth", None)),
        check_vma=False,
    )
```
